512 devices in a mesh: mem: 16 (over z, core), tile: 32 (over x, y).
Axes of the slice: x: 4, y: 8, z: 8, core: 2. Of those that a mesh axis runs over, the one named last changes fastest.
Arguments:
- state: float32 [80, 32, 12960], P('mem', 'tile'), may hold values from -6 to 6
- obs_index: int32 [32, 256], P('tile'), may hold values from 0 to 12959
- obs_count: int32 [32], P('tile'), may hold values from 32 to 256, as said below
- obs_value: float32 [32, 256], P('tile'), may hold values from -8 to 8
- obs_rinv: float32 [32, 256], P('tile'), may hold values from 0.1 to 1
- radius: int32 [32], P('tile'), may hold values from 1 to 2
Outputs:
- analysis: float32 [80, 32, 12960], P('mem', 'tile')
The draws below stay inside these ranges and needn't reach their ends.
Inputs may be any that keep to these rules, and one draw needn't show every extreme that they name: `obs_count`: at most 256; some tile has exactly 256 in every draw.
All inputs are finite; a program needn't handle non-finite values.
Results may differ from the reference program's by a relative error of at most 0.0003.
Values sent between devices are 32-bit elements; how exact they have to be, the bound alone decides.
No kernel may reach another device: no remote copies, remote signals or barrier semaphores. Data moves between devices by JAX's collectives and lax.ppermute only.
A program may use at most 64 MiB of HBM per device.

```python
import math
import jax
import jax.numpy as jnp
from jax import lax

LAT = 288
COLS = 45
BLOCK = 9
SLOTS = 256
HALO = 2
NS_ITERS = 4
MEMBERS = 80
TILES = 32
CELLS_TILE = 12960
N_MEM = 16


def draw_obs_count(key, part):
    base_key = jax.random.fold_in(key, 11)
    order_key = jax.random.fold_in(key, 12)
    base = jax.random.randint(base_key, (TILES,), SLOTS // 8, SLOTS // 3 + 1)
    order = jax.random.permutation(order_key, TILES)
    dense = order < max(1, TILES // 8)
    return jnp.where(dense, SLOTS, base).astype(jnp.int32)


def plant(array, own_key, low, high):
    spot = [jax.random.randint(jax.random.fold_in(own_key, axis), (), 0, length) for axis, length in enumerate(array.shape)]
    widest = array.shape.index(max(array.shape))
    neighbour = spot[:widest] + [(spot[widest] + 1) % array.shape[widest]] + spot[widest + 1:]
    return array.at[tuple(spot)].set(low).at[tuple(neighbour)].set(high)


def block_scale(key, shape, pieces, low, top_value):
    factor_of, own = 1.0, jax.random.fold_in(key, 6)
    for axis_at, shards_of in pieces:
        draws = jnp.exp(jax.random.uniform(jax.random.fold_in(own, axis_at), (shards_of,), jnp.float32, low / len(pieces), top_value / len(pieces)))
        factor_of = factor_of * jnp.repeat(draws, shape[axis_at] // shards_of).reshape([-1 if axis == axis_at else 1 for axis in range(len(shape))])
    return factor_of


def gaussian(own_key, dims, width, most, split=(), held_as=jnp.bfloat16):
    factor_of = block_scale(own_key, dims, split, -0.22, 0.18) if split else 1.0
    entries = jax.random.normal(own_key, dims, jnp.float32) * width * factor_of
    return jnp.minimum(jnp.maximum(entries, -most), most).astype(held_as)


def setup_inputs(seed: int = 0) -> dict:
    arg_keys = jax.random.split(jax.random.key(seed), 7)
    state = gaussian(arg_keys[0], (MEMBERS, TILES, CELLS_TILE), 1.0, 6.0, ((0, 16), (1, 32)), jnp.float32)
    obs_index = plant(jax.random.randint(arg_keys[1], (TILES, SLOTS), 0, LAT * COLS), jax.random.fold_in(arg_keys[1], 1), 0, (LAT * COLS) - 1).astype(jnp.int32)
    obs_count = draw_obs_count(jax.random.fold_in(arg_keys[6], 71), 0)
    obs_value = gaussian(arg_keys[3], (TILES, SLOTS), 1.5, 8.0, ((0, 32),), jnp.float32)
    obs_rinv = jnp.clip(jnp.exp(math.log(1.0) - 2.3025851 * jax.random.uniform(arg_keys[4], (TILES, SLOTS), jnp.float32) ** block_scale(arg_keys[4], (TILES, SLOTS), ((0, 32),), -0.2, 0.2)), 0.1, 1.0)
    radius = plant(jax.random.randint(arg_keys[5], (TILES,), 1, HALO + 1), jax.random.fold_in(arg_keys[5], 1), 1, HALO).astype(jnp.int32)
    return {"state": state, "obs_index": obs_index, "obs_count": obs_count, "obs_value": obs_value, "obs_rinv": obs_rinv, "radius": radius}


highest = lax.Precision.HIGHEST

def block_points(band_id, tile_id, rows_dev):
    half_block = (BLOCK - 1) // 2
    row_blocks = rows_dev // BLOCK
    col_blocks = COLS // BLOCK
    row_ids = band_id * rows_dev + BLOCK * jnp.arange(row_blocks, dtype=jnp.int32) + half_block
    col_ids = tile_id * COLS + BLOCK * jnp.arange(col_blocks, dtype=jnp.int32) + half_block
    point_rows = jnp.broadcast_to(row_ids[:, None], (row_blocks, col_blocks)).reshape(-1).astype(jnp.float32)
    point_cols = jnp.broadcast_to(col_ids[None, :], (row_blocks, col_blocks)).reshape(-1).astype(jnp.float32)
    return (point_rows, point_cols)

def locality(obs_meta, point_rows, point_cols, extent, circle):
    row_gap = jnp.abs(obs_meta[2][None, :] - point_rows[:, None])
    col_gap = jnp.abs(obs_meta[3][None, :] - point_cols[:, None])
    col_gap = jnp.minimum(col_gap, circle - col_gap)
    taper = jnp.maximum(0.0, 1.0 - row_gap / extent) * jnp.maximum(0.0, 1.0 - col_gap / extent)
    return taper * obs_meta[1][None, :]

def accumulate(totals, ens_blk, meta_blk, point_rows, point_cols, extent, circle):
    gram_sum, rhs_sum = totals
    centre = lax.optimization_barrier(jnp.mean(ens_blk, axis=0))
    spread_obs = ens_blk - centre[None, :]
    innovation = meta_blk[0] - centre
    weights = locality(meta_blk, point_rows, point_cols, extent, circle)
    weighted = weights[:, None, :] * spread_obs[None, :, :]
    gram_sum = gram_sum + jnp.einsum('pkj,lj->pkl', weighted, spread_obs, precision=highest)
    rhs_sum = rhs_sum + jnp.einsum('pkj,j->pk', weighted, innovation, precision=highest)
    return (gram_sum, rhs_sum)

def transform(gram_sum, rhs_sum, members):
    identity = jnp.eye(members, dtype=gram_sum.dtype)
    gram_full = gram_sum + (members - 1.0) * identity[None]
    frob_norm = jnp.sqrt(lax.optimization_barrier(jnp.sum(gram_full * gram_full, axis=(1, 2))))
    iterate = gram_full / frob_norm[:, None, None]
    inv_root = jnp.broadcast_to(identity, gram_full.shape)
    for sweep in range(NS_ITERS):
        middle = 1.5 * identity[None] - 0.5 * jnp.einsum('pij,pjk->pik', inv_root, iterate, precision=highest)
        iterate = jnp.einsum('pij,pjk->pik', iterate, middle, precision=highest)
        inv_root = jnp.einsum('pij,pjk->pik', middle, inv_root, precision=highest)
    inv_root = inv_root / jnp.sqrt(frob_norm)[:, None, None]
    inner = jnp.einsum('pij,pj->pi', inv_root, rhs_sum, precision=highest)
    mean_shift = jnp.einsum('pij,pj->pi', inv_root, inner, precision=highest)
    return jnp.sqrt(members - 1.0) * inv_root + mean_shift[:, :, None]

def apply_mix(band_state, mixing, rows_dev):
    members = band_state.shape[0]
    row_blocks = rows_dev // BLOCK
    col_blocks = COLS // BLOCK
    cell_grid = band_state.reshape(members, row_blocks, BLOCK, col_blocks, BLOCK)
    centre = lax.optimization_barrier(jnp.mean(cell_grid, axis=0))
    spread_state = cell_grid - centre[None]
    mix_blocks = mixing.reshape(row_blocks, col_blocks, members, members)
    result = jnp.einsum('ablk,laibj->kaibj', mix_blocks, spread_state, precision=highest) + centre[None]
    return result.reshape(members, rows_dev * COLS)

def reference(state, obs_index, obs_count, obs_value, obs_rinv, radius):
    members = state.shape[0]
    tile_count = state.shape[1]
    cell_count = state.shape[2]
    rows_dev = LAT // N_MEM
    band_cells = rows_dev * COLS
    circle = 1.0 * COLS * tile_count
    ens_obs = jax.vmap(lambda field_rows, cell_ids: field_rows[:, cell_ids], in_axes=(1, 0), out_axes=1)(state, obs_index)
    slot_ids = jnp.arange(SLOTS, dtype=jnp.int32)
    is_live = slot_ids[None, :] < obs_count[:, None]
    rinv_live = jnp.where(is_live, obs_rinv, 0.0)
    tile_ids = jnp.arange(tile_count, dtype=jnp.int32)
    obs_row = (obs_index // COLS).astype(jnp.float32)
    obs_col = (obs_index % COLS + tile_ids[:, None] * COLS).astype(jnp.float32)
    obs_meta = jnp.stack([obs_value, rinv_live, obs_row, obs_col])
    stacked = jnp.concatenate([ens_obs, obs_meta], axis=0)
    offsets = jnp.arange(-HALO, HALO + 1, dtype=jnp.int32)

    def per_tile(tile_id):
        window = stacked[:, (tile_id + offsets) % tile_count, :].reshape(members + 4, -1)
        ens_win = window[:members]
        meta_win = window[members:]
        extent = (radius[tile_id] * COLS).astype(jnp.float32)
        tile_state = lax.dynamic_index_in_dim(state, tile_id, axis=1, keepdims=False)
        band_rows = tile_state.reshape(members, N_MEM, band_cells).transpose(1, 0, 2)

        def per_band(pair_item):
            band_id, band_state = pair_item
            point_rows, point_cols = block_points(band_id, tile_id, rows_dev)
            points = point_rows.shape[0]
            totals = (jnp.zeros((points, members, members), jnp.float32), jnp.zeros((points, members), jnp.float32))
            gram_sum, rhs_sum = accumulate(totals, ens_win, meta_win, point_rows, point_cols, extent, circle)
            mixing = transform(gram_sum, rhs_sum, members)
            return apply_mix(band_state, mixing, rows_dev)
        result = lax.map(per_band, (jnp.arange(N_MEM, dtype=jnp.int32), band_rows))
        return result.transpose(1, 0, 2).reshape(members, cell_count)
    outcome = lax.map(per_tile, tile_ids)
    return outcome.transpose(1, 0, 2)
```

```python
import jax
import jax.numpy as jnp
from jax import lax
from jax.experimental import pallas as pl
from jax.experimental.pallas import tpu as pltpu
from jax.sharding import PartitionSpec as P

COLS = 45
BLOCK = 9
HALO = 2
NS_ITERS = 4
LANES = 128
PIECE_ROWS = 88


def halves(x):
    high = x.astype(jnp.bfloat16)
    low = (x - high.astype(jnp.float32)).astype(jnp.bfloat16)
    return high, low


def dot_nn(a, b):
    return lax.dot_general(a, b, (((1,), (0,)), ((), ())), preferred_element_type=jnp.float32)


def dot_nt(a, b):
    return lax.dot_general(a, b, (((1,), (1,)), ((), ())), preferred_element_type=jnp.float32)


def take_body(state_ref, index_ref, out_ref, rows_ref):
    mem_dev, _, cells = state_ref.shape
    whole = cells // LANES
    rest = cells - whole * LANES
    rows_ref[:, whole // 8 * 8 :, :] = jnp.zeros(
        (mem_dev, rows_ref.shape[1] - whole // 8 * 8, LANES), jnp.float32
    )
    for m in range(mem_dev):
        for c in range(whole):
            rows_ref[m, c : c + 1, :] = state_ref[m, :, c * LANES : (c + 1) * LANES]
        if rest:
            rows_ref[m, whole : whole + 1, 0:rest] = state_ref[m, :, whole * LANES : cells]
    index = index_ref[0:1, :]
    slots = index.shape[1]
    row_of = index // LANES
    lane_of = index - row_of * LANES
    spot = lax.broadcasted_iota(jnp.int32, (LANES, slots), 0)
    pick = jnp.where(spot == row_of, 1.0, 0.0).astype(jnp.bfloat16)
    found = []
    for m in range(mem_dev):
        flipped = rows_ref[m].T
        high = flipped.astype(jnp.bfloat16)
        left = flipped - high.astype(jnp.float32)
        mid = left.astype(jnp.bfloat16)
        low = (left - mid.astype(jnp.float32)).astype(jnp.bfloat16)
        value = (dot_nn(high, pick) + dot_nn(mid, pick)) + dot_nn(low, pick)
        found.append(jnp.sum(jnp.where(spot == lane_of, value, 0.0), axis=0, keepdims=True))
    own = jnp.concatenate(found, axis=0)
    for copy in range(out_ref.shape[0]):
        out_ref[copy] = own


def take_cells(state, index, copies):
    mem_dev, _, cells = state.shape
    return pl.pallas_call(
        take_body,
        out_shape=jax.ShapeDtypeStruct((copies, mem_dev, index.shape[1]), jnp.float32),
        scratch_shapes=[pltpu.VMEM((mem_dev, LANES, LANES), jnp.float32)],
        name="take_cells",
    )(state, index)


def analysis_body(
    radius_ref, band_ref, tile_ref, own_ref, up1_ref, dn1_ref, up2_ref, dn2_ref, state_ref,
    out_ref, ens_ref, weight_ref, live_ref, gram_ref, iter_ref, root_ref, mix_ref, *, circle, rows_dev
):
    members = state_ref.shape[0]
    slots = own_ref.shape[1]
    per_piece = slots // LANES
    col_blocks = COLS // BLOCK
    row_blocks = rows_dev // BLOCK
    points = row_blocks * col_blocks
    half_block = (BLOCK - 1) // 2
    pad_points = 16
    pieces = [own_ref, up1_ref, dn1_ref, up2_ref, dn2_ref]
    blocks = len(pieces) * per_piece
    extent = (radius_ref[0] * COLS).astype(jnp.float32)
    point = lax.broadcasted_iota(jnp.int32, (pad_points, LANES), 0)
    point_row = jnp.zeros((pad_points, LANES), jnp.int32)
    for r in range(1, row_blocks):
        point_row = point_row + jnp.where(point >= r * col_blocks, 1, 0)
    point_col = point - point_row * col_blocks
    prow = (band_ref[0] * rows_dev + BLOCK * point_row + half_block).astype(jnp.float32)
    pcol = (tile_ref[0] * COLS + BLOCK * point_col + half_block).astype(jnp.float32)
    for b in range(blocks):
        ref = pieces[b // per_piece]
        lanes = slice((b % per_piece) * LANES, (b % per_piece + 1) * LANES)
        ens = ref[0:members, lanes]
        centre = jnp.sum(ens, axis=0, keepdims=True) / members
        ens_ref[b, 0:members, :] = ens - centre
        meta = ref[members : members + 4, lanes]
        ens_ref[b, members : members + 1, :] = meta[0:1] - centre
        row_gap = jnp.abs(meta[2:3] - prow)
        col_gap = jnp.abs(meta[3:4] - pcol)
        col_gap = jnp.minimum(col_gap, circle - col_gap)
        taper = jnp.maximum(0.0, 1.0 - row_gap / extent) * jnp.maximum(0.0, 1.0 - col_gap / extent)
        weight = taper * meta[1:2]
        weight_ref[b] = weight
        live_ref[b] = (jnp.max(weight) > 0.0).astype(jnp.int32)
    gram_ref[...] = jnp.zeros(gram_ref.shape, jnp.float32)
    fill = jnp.zeros((LANES - members, 2 * LANES), jnp.bfloat16)
    blank = jnp.zeros((members, LANES), jnp.bfloat16)

    def visit(b, carry):
        @pl.when(live_ref[b] > 0)
        def _():
            spread = ens_ref[b, 0:members, :]
            innovation = ens_ref[b, members : members + 1, :]
            weight = weight_ref[b]
            high, low = halves(spread)
            right = jnp.concatenate(
                [
                    jnp.concatenate([high, high], axis=1),
                    fill,
                    jnp.concatenate([low, blank], axis=1),
                    fill,
                ],
                axis=0,
            )
            left = []
            for p in range(points):
                left.append(jnp.concatenate(halves(weight[p : p + 1] * spread), axis=1))
            left.append(jnp.concatenate(halves(weight * innovation), axis=1))
            gram_ref[...] += dot_nt(jnp.concatenate(left, axis=0), right)

        return carry

    lax.fori_loop(0, blocks, visit, 0)

    row_id = lax.broadcasted_iota(jnp.int32, (members, LANES), 0)
    lane_id = lax.broadcasted_iota(jnp.int32, (members, LANES), 1)
    identity = jnp.where(row_id == lane_id, 1.0, 0.0)
    middle_id = 1.5 * identity

    def left_of(parts):
        return jnp.concatenate(parts, axis=1)

    def right_of(parts):
        high, low = parts
        return jnp.concatenate(
            [
                jnp.concatenate([high, low], axis=1),
                fill,
                jnp.concatenate([high, blank], axis=1),
                fill,
            ],
            axis=0,
        )

    def folded(x):
        return x[:, :LANES] + x[:, LANES:]

    norms = []
    for p in range(points):
        gram = folded(gram_ref[p * members : (p + 1) * members, :]) + (members - 1.0) * identity
        squares = jnp.sum(jnp.sum(gram * gram, axis=0, keepdims=True), axis=1, keepdims=True)
        norm = jnp.sqrt(squares)
        norms.append(norm)
        iter_ref[p] = gram / norm
    for p in range(points):
        iterate = iter_ref[p]
        middle = middle_id - 0.5 * iterate
        iter_ref[p] = folded(dot_nn(left_of(halves(iterate)), right_of(halves(middle))))
        root_ref[p] = middle
    for sweep in range(1, NS_ITERS):
        last = sweep == NS_ITERS - 1
        for p in range(points):
            root = halves(root_ref[p])
            iterate = halves(iter_ref[p])
            product = folded(dot_nn(left_of(root), right_of(iterate)))
            middle = right_of(halves(middle_id - 0.5 * product))
            if last:
                root_ref[p] = folded(dot_nn(left_of(root), middle))
            else:
                both = jnp.concatenate([left_of(root), left_of(iterate)], axis=0)
                both = folded(dot_nn(both, middle))
                root_ref[p] = both[0:members]
                iter_ref[p] = both[members:]
    rhs_all = folded(gram_ref[points * members : points * members + pad_points, :])
    scale = (members - 1.0) ** 0.5
    for p in range(points):
        root = root_ref[p] / jnp.sqrt(norms[p])
        inner = jnp.sum(root * rhs_all[p : p + 1], axis=1, keepdims=True)
        shift = jnp.sum(root * inner, axis=0, keepdims=True)
        high, low = halves(scale * root + shift)
        mix_ref[p * members : (p + 1) * members, 0:LANES] = high
        mix_ref[p * members : (p + 1) * members, LANES:] = low

    cells = state_ref.shape[2]
    state = state_ref[:, 0, :]
    centre = jnp.sum(state, axis=0, keepdims=True) / members
    spread = state - centre
    wide = -(-cells // LANES) * LANES
    band_half = BLOCK * COLS
    results = []
    for r in range(row_blocks):
        start = r * band_half // LANES * LANES
        stop = min(wide, -(-(r + 1) * band_half // LANES) * LANES)
        part = spread[:, start : min(stop, cells)]
        width = part.shape[1]
        high, low = halves(part)
        hole = jnp.zeros((LANES - members, width), jnp.bfloat16)
        top = jnp.concatenate([high, hole, high, hole], axis=0)
        bottom = jnp.concatenate([low, hole], axis=0)
        mix = mix_ref[r * col_blocks * members : (r + 1) * col_blocks * members, :]
        product = dot_nn(mix, top) + dot_nn(mix[:, :LANES], bottom)
        cell = lax.broadcasted_iota(jnp.int32, (members, width), 1) + start
        column = lax.rem(cell, COLS) // BLOCK
        result = centre[:, start : start + width]
        for cb in range(col_blocks):
            result = result + jnp.where(column == cb, product[cb * members : (cb + 1) * members], 0.0)
        results.append((start, width, cell, result))
    if row_blocks == 2:
        (s0, w0, c0, r0), (s1, w1, c1, r1) = results
        out_ref[:, 0, 0:s1] = r0[:, 0:s1]
        joint = jnp.where(c0[:, s1:] < band_half, r0[:, s1:], r1[:, 0 : s0 + w0 - s1])
        out_ref[:, 0, s1 : s0 + w0] = joint
        out_ref[:, 0, s0 + w0 : cells] = r1[:, s0 + w0 - s1 :]


def analysis(radius, band_id, tile_id, pieces, state, circle, rows_dev):
    members = state.shape[0]
    slots = pieces[0].shape[1]
    blocks = len(pieces) * slots // LANES
    points = rows_dev // BLOCK * (COLS // BLOCK)
    smem = pl.BlockSpec(memory_space=pltpu.SMEM)
    vmem = pl.BlockSpec(memory_space=pltpu.VMEM)

    def body(*refs):
        analysis_body(*refs, circle=circle, rows_dev=rows_dev)

    return pl.pallas_call(
        body,
        out_shape=jax.ShapeDtypeStruct(state.shape, jnp.float32),
        in_specs=[smem] * 3 + [vmem] * (len(pieces) + 1),
        out_specs=vmem,
        scratch_shapes=[
            pltpu.VMEM((blocks, PIECE_ROWS, LANES), jnp.float32),
            pltpu.VMEM((blocks, 16, LANES), jnp.float32),
            pltpu.SMEM((blocks,), jnp.int32),
            pltpu.VMEM((points * members + 16, 2 * LANES), jnp.float32),
            pltpu.VMEM((points, members, LANES), jnp.float32),
            pltpu.VMEM((points, members, LANES), jnp.float32),
            pltpu.VMEM((points * members, 2 * LANES), jnp.bfloat16),
        ],
        name="analysis",
    )(radius, band_id, tile_id, *pieces, state)


def shifted(block, axis, distance):
    devices = range(lax.axis_size(axis))
    route = [((i - distance) % len(devices), i) for i in devices]
    return lax.ppermute(block, axis, route)


def shards(state, obs_index, obs_count, obs_value, obs_rinv, radius):
    groups = lax.axis_size("mem")
    tile_count = lax.axis_size("tile")
    mem_dev = state.shape[0]
    cell_count = state.shape[2]
    members = mem_dev * groups
    band_cells = cell_count // groups
    rows_dev = band_cells // COLS
    circle = 1.0 * COLS * tile_count
    tile_id = lax.axis_index("tile")
    band_id = lax.axis_index("mem")
    slot_count = obs_index.shape[1]
    cell_index = obs_index[0]
    copies = take_cells(state, obs_index, groups)
    ensemble = lax.all_to_all(copies, "mem", 0, 0, tiled=True).reshape(members, slot_count)
    chunks = state.reshape(mem_dev, groups, band_cells).transpose(1, 0, 2)
    chunks = chunks.reshape(members, 1, band_cells)
    band_state = lax.all_to_all(chunks, "mem", 0, 0, tiled=True)
    slot_ids = jnp.arange(slot_count, dtype=jnp.int32)
    rinv_live = jnp.where(slot_ids < obs_count[0], obs_rinv[0], 0.0)
    obs_row = (cell_index // COLS).astype(jnp.float32)
    obs_col = (cell_index % COLS + tile_id * COLS).astype(jnp.float32)
    obs_meta = jnp.stack([obs_value[0], rinv_live, obs_row, obs_col])
    local_rows = jnp.concatenate([ensemble, obs_meta], axis=0)
    offsets = [distance * direction for distance in range(1, HALO + 1) for direction in (1, -1)]
    pieces = [local_rows] + [shifted(local_rows, "tile", offset) for offset in offsets]
    result = analysis(
        radius, band_id.reshape(1), tile_id.reshape(1), pieces, band_state, circle, rows_dev
    )
    returned = lax.all_to_all(result, "mem", 0, 0, tiled=True)
    returned = returned.reshape(groups, mem_dev, band_cells).transpose(1, 0, 2)
    return returned.reshape(mem_dev, 1, cell_count)


def solution(mesh):
    in_specs = (
        P("mem", "tile", None),
        P("tile", None),
        P("tile"),
        P("tile", None),
        P("tile", None),
        P("tile"),
    )
    out_specs = P("mem", "tile", None)
    return jax.shard_map(shards, mesh=mesh, in_specs=in_specs, out_specs=out_specs, check_vma=False)
```

```python
import jax
import jax.numpy as jnp
from jax import lax
from jax.experimental import pallas as pl
from jax.experimental.pallas import tpu as pltpu
from jax.sharding import PartitionSpec as P

COLS = 45
BLOCK = 9
HALO = 2
NS_ITERS = 4
LANES = 128
PIECE_ROWS = 88


def halves(x):
    high = x.astype(jnp.bfloat16)
    low = (x - high.astype(jnp.float32)).astype(jnp.bfloat16)
    return high, low


def dot_nn(a, b):
    return lax.dot_general(a, b, (((1,), (0,)), ((), ())), preferred_element_type=jnp.float32)


def dot_nt(a, b):
    return lax.dot_general(a, b, (((1,), (1,)), ((), ())), preferred_element_type=jnp.float32)


def take_body(count_ref, tile_ref, state_ref, index_ref, value_ref, rinv_ref, out_ref, meta_ref, rows_ref):
    mem_dev, _, cells = state_ref.shape
    whole = cells // LANES
    rest = cells - whole * LANES
    rows_ref[:, whole // 8 * 8 :, :] = jnp.zeros(
        (mem_dev, rows_ref.shape[1] - whole // 8 * 8, LANES), jnp.float32
    )
    for m in range(mem_dev):
        for c in range(whole):
            rows_ref[m, c : c + 1, :] = state_ref[m, :, c * LANES : (c + 1) * LANES]
        if rest:
            rows_ref[m, whole : whole + 1, 0:rest] = state_ref[m, :, whole * LANES : cells]
    index = index_ref[0:1, :]
    slots = index.shape[1]
    row_of = index // LANES
    lane_of = index - row_of * LANES
    spot = lax.broadcasted_iota(jnp.int32, (LANES, slots), 0)
    pick = jnp.where(spot == row_of, 1.0, 0.0).astype(jnp.bfloat16)
    found = []
    for m in range(mem_dev):
        flipped = rows_ref[m].T
        high = flipped.astype(jnp.bfloat16)
        left = flipped - high.astype(jnp.float32)
        mid = left.astype(jnp.bfloat16)
        low = (left - mid.astype(jnp.float32)).astype(jnp.bfloat16)
        value = (dot_nn(high, pick) + dot_nn(mid, pick)) + dot_nn(low, pick)
        found.append(jnp.sum(jnp.where(spot == lane_of, value, 0.0), axis=0, keepdims=True))
    own = jnp.concatenate(found, axis=0)
    for copy in range(out_ref.shape[0]):
        out_ref[copy] = own
    slot = lax.broadcasted_iota(jnp.int32, (1, slots), 1)
    obs_row = index // COLS
    obs_col = index - obs_row * COLS + tile_ref[0] * COLS
    meta_ref[...] = jnp.concatenate(
        [
            value_ref[...],
            jnp.where(slot < count_ref[0], rinv_ref[...], 0.0),
            obs_row.astype(jnp.float32),
            obs_col.astype(jnp.float32),
            jnp.zeros((4, slots), jnp.float32),
        ],
        axis=0,
    )


def on_chip(x):
    return pltpu.with_memory_space_constraint(x, pltpu.VMEM)


def take_cells(count, tile_id, state, index, value, rinv, copies):
    mem_dev, _, cells = state.shape
    slots = index.shape[1]
    smem = pl.BlockSpec(memory_space=pltpu.SMEM)
    vmem = pl.BlockSpec(memory_space=pltpu.VMEM)
    return pl.pallas_call(
        take_body,
        out_shape=(
            pltpu.VMEM((copies, mem_dev, slots), jnp.float32),
            pltpu.VMEM((8, slots), jnp.float32),
        ),
        in_specs=[smem] * 2 + [vmem] * 4,
        out_specs=(vmem, vmem),
        scratch_shapes=[pltpu.VMEM((mem_dev, LANES, LANES), jnp.float32)],
        name="take_cells",
    )(count, tile_id, state, index, value, rinv)


def analysis_body(
    radius_ref, band_ref, tile_ref, own_ref, near_ref, state_ref, out_ref,
    ens_ref, weight_ref, live_ref, gram_ref, iter_ref, root_ref, mix_ref, *, circle, rows_dev
):
    members = state_ref.shape[0]
    slots = own_ref.shape[1]
    per_piece = slots // LANES
    col_blocks = COLS // BLOCK
    row_blocks = rows_dev // BLOCK
    points = row_blocks * col_blocks
    half_block = (BLOCK - 1) // 2
    pad_points = 16
    pieces = [own_ref]
    for core in range(near_ref.shape[0]):
        for start in range(0, near_ref.shape[1], PIECE_ROWS):
            pieces.append(near_ref.at[core, start : start + PIECE_ROWS])
    blocks = len(pieces) * per_piece
    extent = (radius_ref[0] * COLS).astype(jnp.float32)
    point = lax.broadcasted_iota(jnp.int32, (pad_points, LANES), 0)
    point_row = jnp.zeros((pad_points, LANES), jnp.int32)
    for r in range(1, row_blocks):
        point_row = point_row + jnp.where(point >= r * col_blocks, 1, 0)
    point_col = point - point_row * col_blocks
    prow = (band_ref[0] * rows_dev + BLOCK * point_row + half_block).astype(jnp.float32)
    pcol = (tile_ref[0] * COLS + BLOCK * point_col + half_block).astype(jnp.float32)
    for b in range(blocks):
        ref = pieces[b // per_piece]
        lanes = slice((b % per_piece) * LANES, (b % per_piece + 1) * LANES)
        ens = ref[0:members, lanes]
        centre = jnp.sum(ens, axis=0, keepdims=True) / members
        ens_ref[b, 0:members, :] = ens - centre
        meta = ref[members : members + 4, lanes]
        ens_ref[b, members : members + 1, :] = meta[0:1] - centre
        row_gap = jnp.abs(meta[2:3] - prow)
        col_gap = jnp.abs(meta[3:4] - pcol)
        col_gap = jnp.minimum(col_gap, circle - col_gap)
        taper = jnp.maximum(0.0, 1.0 - row_gap / extent) * jnp.maximum(0.0, 1.0 - col_gap / extent)
        weight = taper * meta[1:2]
        weight_ref[b] = weight
        live_ref[b] = (jnp.max(weight) > 0.0).astype(jnp.int32)
    gram_ref[...] = jnp.zeros(gram_ref.shape, jnp.float32)
    fill = jnp.zeros((LANES - members, 2 * LANES), jnp.bfloat16)
    blank = jnp.zeros((members, LANES), jnp.bfloat16)

    def visit(b, carry):
        @pl.when(live_ref[b] > 0)
        def _():
            spread = ens_ref[b, 0:members, :]
            innovation = ens_ref[b, members : members + 1, :]
            weight = weight_ref[b]
            high, low = halves(spread)
            right = jnp.concatenate(
                [
                    jnp.concatenate([high, high], axis=1),
                    fill,
                    jnp.concatenate([low, blank], axis=1),
                    fill,
                ],
                axis=0,
            )
            left = []
            for p in range(points):
                left.append(jnp.concatenate(halves(weight[p : p + 1] * spread), axis=1))
            left.append(jnp.concatenate(halves(weight * innovation), axis=1))
            gram_ref[...] += dot_nt(jnp.concatenate(left, axis=0), right)

        return carry

    lax.fori_loop(0, blocks, visit, 0)

    row_id = lax.broadcasted_iota(jnp.int32, (members, LANES), 0)
    lane_id = lax.broadcasted_iota(jnp.int32, (members, LANES), 1)
    identity = jnp.where(row_id == lane_id, 1.0, 0.0)
    middle_id = 1.5 * identity

    def left_of(parts):
        return jnp.concatenate(parts, axis=1)

    def right_of(parts):
        high, low = parts
        return jnp.concatenate(
            [
                jnp.concatenate([high, low], axis=1),
                fill,
                jnp.concatenate([high, blank], axis=1),
                fill,
            ],
            axis=0,
        )

    def folded(x):
        return x[:, :LANES] + x[:, LANES:]

    norms = []
    for p in range(points):
        gram = folded(gram_ref[p * members : (p + 1) * members, :]) + (members - 1.0) * identity
        squares = jnp.sum(jnp.sum(gram * gram, axis=0, keepdims=True), axis=1, keepdims=True)
        norm = jnp.sqrt(squares)
        norms.append(norm)
        iter_ref[p] = gram / norm
    for p in range(points):
        iterate = iter_ref[p]
        middle = middle_id - 0.5 * iterate
        iter_ref[p] = folded(dot_nn(left_of(halves(iterate)), right_of(halves(middle))))
        root_ref[p] = middle
    for sweep in range(1, NS_ITERS):
        last = sweep == NS_ITERS - 1
        for p in range(points):
            root = halves(root_ref[p])
            iterate = halves(iter_ref[p])
            product = folded(dot_nn(left_of(root), right_of(iterate)))
            middle = right_of(halves(middle_id - 0.5 * product))
            if last:
                root_ref[p] = folded(dot_nn(left_of(root), middle))
            else:
                both = jnp.concatenate([left_of(root), left_of(iterate)], axis=0)
                both = folded(dot_nn(both, middle))
                root_ref[p] = both[0:members]
                iter_ref[p] = both[members:]
    rhs_all = folded(gram_ref[points * members : points * members + pad_points, :])
    scale = (members - 1.0) ** 0.5
    for p in range(points):
        root = root_ref[p] / jnp.sqrt(norms[p])
        inner = jnp.sum(root * rhs_all[p : p + 1], axis=1, keepdims=True)
        shift = jnp.sum(root * inner, axis=0, keepdims=True)
        high, low = halves(scale * root + shift)
        mix_ref[p * members : (p + 1) * members, 0:LANES] = high
        mix_ref[p * members : (p + 1) * members, LANES:] = low

    cells = state_ref.shape[2]
    state = state_ref[:, 0, :]
    centre = jnp.sum(state, axis=0, keepdims=True) / members
    spread = state - centre
    wide = -(-cells // LANES) * LANES
    band_half = BLOCK * COLS
    results = []
    for r in range(row_blocks):
        start = r * band_half // LANES * LANES
        stop = min(wide, -(-(r + 1) * band_half // LANES) * LANES)
        part = spread[:, start : min(stop, cells)]
        width = part.shape[1]
        high, low = halves(part)
        hole = jnp.zeros((LANES - members, width), jnp.bfloat16)
        top = jnp.concatenate([high, hole, high, hole], axis=0)
        bottom = jnp.concatenate([low, hole], axis=0)
        mix = mix_ref[r * col_blocks * members : (r + 1) * col_blocks * members, :]
        product = dot_nn(mix, top) + dot_nn(mix[:, :LANES], bottom)
        cell = lax.broadcasted_iota(jnp.int32, (members, width), 1) + start
        column = lax.rem(cell, COLS) // BLOCK
        result = centre[:, start : start + width]
        for cb in range(col_blocks):
            result = result + jnp.where(column == cb, product[cb * members : (cb + 1) * members], 0.0)
        results.append((start, width, cell, result))
    if row_blocks == 2:
        (s0, w0, c0, r0), (s1, w1, c1, r1) = results
        out_ref[:, 0, 0:s1] = r0[:, 0:s1]
        joint = jnp.where(c0[:, s1:] < band_half, r0[:, s1:], r1[:, 0 : s0 + w0 - s1])
        out_ref[:, 0, s1 : s0 + w0] = joint
        out_ref[:, 0, s0 + w0 : cells] = r1[:, s0 + w0 - s1 :]


def analysis(radius, band_id, tile_id, own, near, state, circle, rows_dev):
    members = state.shape[0]
    slots = own.shape[1]
    blocks = (1 + near.shape[0] * (near.shape[1] // PIECE_ROWS)) * slots // LANES
    points = rows_dev // BLOCK * (COLS // BLOCK)
    smem = pl.BlockSpec(memory_space=pltpu.SMEM)
    vmem = pl.BlockSpec(memory_space=pltpu.VMEM)

    def body(*refs):
        analysis_body(*refs, circle=circle, rows_dev=rows_dev)

    return pl.pallas_call(
        body,
        out_shape=pltpu.VMEM(state.shape, jnp.float32),
        in_specs=[smem] * 3 + [vmem] * 3,
        out_specs=vmem,
        scratch_shapes=[
            pltpu.VMEM((blocks, PIECE_ROWS, LANES), jnp.float32),
            pltpu.VMEM((blocks, 16, LANES), jnp.float32),
            pltpu.SMEM((blocks,), jnp.int32),
            pltpu.VMEM((points * members + 16, 2 * LANES), jnp.float32),
            pltpu.VMEM((points, members, LANES), jnp.float32),
            pltpu.VMEM((points, members, LANES), jnp.float32),
            pltpu.VMEM((points * members, 2 * LANES), jnp.bfloat16),
        ],
        name="analysis",
    )(radius, band_id, tile_id, on_chip(own), on_chip(near), on_chip(state))


def fetched(block, distance):
    tiles = lax.axis_size("tile")
    route = []
    for group in range(lax.axis_size("mem")):
        step = distance if group % 2 == 0 else -distance
        route += [(group * tiles + (t - step) % tiles, group * tiles + t) for t in range(tiles)]
    return lax.ppermute(block, ("mem", "tile"), route)


def shards(state, obs_index, obs_count, obs_value, obs_rinv, radius):
    groups = lax.axis_size("mem")
    tile_count = lax.axis_size("tile")
    mem_dev = state.shape[0]
    cell_count = state.shape[2]
    members = mem_dev * groups
    band_cells = cell_count // groups
    rows_dev = band_cells // COLS
    circle = 1.0 * COLS * tile_count
    tile_id = lax.axis_index("tile")
    band_id = lax.axis_index("mem")
    slot_count = obs_index.shape[1]
    tile_at = tile_id.reshape(1)
    copies, meta = take_cells(obs_count, tile_at, state, obs_index, obs_value, obs_rinv, groups)
    ensemble = lax.all_to_all(copies, "mem", 0, 0, tiled=True).reshape(members, slot_count)
    chunks = state.reshape(mem_dev, groups, band_cells).transpose(1, 0, 2)
    chunks = chunks.reshape(members, 1, band_cells)
    band_state = lax.all_to_all(chunks, "mem", 0, 0, tiled=True)
    own = jnp.concatenate([ensemble, meta], axis=0)
    half = jnp.concatenate([fetched(own, distance) for distance in range(1, HALO + 1)], axis=0)
    pairs = [[group, group + 1] for group in range(0, groups, 2)]
    near = lax.all_gather(half, "mem", axis_index_groups=pairs)
    result = analysis(radius, band_id.reshape(1), tile_at, own, near, band_state, circle, rows_dev)
    returned = lax.all_to_all(result, "mem", 0, 0, tiled=True)
    returned = returned.reshape(groups, mem_dev, band_cells).transpose(1, 0, 2)
    return returned.reshape(mem_dev, 1, cell_count)


def solution(mesh):
    in_specs = (
        P("mem", "tile", None),
        P("tile", None),
        P("tile"),
        P("tile", None),
        P("tile", None),
        P("tile"),
    )
    out_specs = P("mem", "tile", None)
    return jax.shard_map(shards, mesh=mesh, in_specs=in_specs, out_specs=out_specs, check_vma=False)
```

```python
import jax
import jax.numpy as jnp
from jax import lax
from jax.experimental import pallas as pl
from jax.experimental.pallas import tpu as pltpu
from jax.sharding import PartitionSpec as P


COLS = 45
BLOCK = 9
HALO = 2
NS_ITERS = 4
LANES = 128
PIECE_ROWS = 88


def halves(x):
    high = x.astype(jnp.bfloat16)
    low = (x - high.astype(jnp.float32)).astype(jnp.bfloat16)
    return high, low


def dot_nn(a, b):
    return lax.dot_general(a, b, (((1,), (0,)), ((), ())), preferred_element_type=jnp.float32)


def dot_nt(a, b):
    return lax.dot_general(a, b, (((1,), (1,)), ((), ())), preferred_element_type=jnp.float32)


def take_body(count_ref, tile_ref, state_ref, index_ref, value_ref, rinv_ref, out_ref, meta_ref, rows_ref):
    mem_dev, _, cells = state_ref.shape
    whole = cells // LANES
    rest = cells - whole * LANES
    rows_ref[:, whole // 8 * 8 :, :] = jnp.zeros(
        (mem_dev, rows_ref.shape[1] - whole // 8 * 8, LANES), jnp.float32
    )
    for m in range(mem_dev):
        for c in range(whole):
            rows_ref[m, c : c + 1, :] = state_ref[m, :, c * LANES : (c + 1) * LANES]
        if rest:
            rows_ref[m, whole : whole + 1, 0:rest] = state_ref[m, :, whole * LANES : cells]
    index = index_ref[0:1, :]
    slots = index.shape[1]
    row_of = index // LANES
    lane_of = index - row_of * LANES
    spot = lax.broadcasted_iota(jnp.int32, (LANES, slots), 0)
    pick = jnp.where(spot == row_of, 1.0, 0.0).astype(jnp.bfloat16)
    found = []
    for m in range(mem_dev):
        flipped = rows_ref[m].T
        high = flipped.astype(jnp.bfloat16)
        left = flipped - high.astype(jnp.float32)
        mid = left.astype(jnp.bfloat16)
        low = (left - mid.astype(jnp.float32)).astype(jnp.bfloat16)
        value = (dot_nn(high, pick) + dot_nn(mid, pick)) + dot_nn(low, pick)
        found.append(jnp.sum(jnp.where(spot == lane_of, value, 0.0), axis=0, keepdims=True))
    own = jnp.concatenate(found, axis=0)
    for copy in range(out_ref.shape[0]):
        out_ref[copy] = own
    slot = lax.broadcasted_iota(jnp.int32, (1, slots), 1)
    obs_row = index // COLS
    obs_col = index - obs_row * COLS + tile_ref[0] * COLS
    meta_ref[...] = jnp.concatenate(
        [
            value_ref[...],
            jnp.where(slot < count_ref[0], rinv_ref[...], 0.0),
            obs_row.astype(jnp.float32),
            obs_col.astype(jnp.float32),
            jnp.zeros((4, slots), jnp.float32),
        ],
        axis=0,
    )


def on_chip(x):
    return pltpu.with_memory_space_constraint(x, pltpu.VMEM)


def take_cells(count, tile_id, state, index, value, rinv, copies):
    mem_dev, _, _ = state.shape
    slots = index.shape[1]
    smem = pl.BlockSpec(memory_space=pltpu.SMEM)
    vmem = pl.BlockSpec(memory_space=pltpu.VMEM)
    return pl.pallas_call(
        take_body,
        out_shape=(
            pltpu.VMEM((copies, mem_dev, slots), jnp.float32),
            pltpu.VMEM((8, slots), jnp.float32),
        ),
        in_specs=[smem] * 2 + [vmem] * 4,
        out_specs=(vmem, vmem),
        scratch_shapes=[pltpu.VMEM((mem_dev, LANES, LANES), jnp.float32)],
        name="take_cells",
    )(count, tile_id, state, index, value, rinv)


def mixing_body(
    extent_ref, band_ref, tile_ref, own_ref, near_ref, mix_ref,
    ens_ref, weight_ref, live_ref, gram_ref, iter_ref, root_ref, *, members, circle, rows_dev
):
    slots = own_ref.shape[1]
    per_piece = slots // LANES
    col_blocks = COLS // BLOCK
    row_blocks = rows_dev // BLOCK
    points = row_blocks * col_blocks
    half_block = (BLOCK - 1) // 2
    pad_points = 16
    pieces = [own_ref]
    for core in range(near_ref.shape[0]):
        for start in range(0, near_ref.shape[1], PIECE_ROWS):
            pieces.append(near_ref.at[core, start : start + PIECE_ROWS])
    blocks = len(pieces) * per_piece
    extent = extent_ref[0]
    point = lax.broadcasted_iota(jnp.int32, (pad_points, LANES), 0)
    point_row = jnp.zeros((pad_points, LANES), jnp.int32)
    for r in range(1, row_blocks):
        point_row = point_row + jnp.where(point >= r * col_blocks, 1, 0)
    point_col = point - point_row * col_blocks
    prow = (band_ref[0] * rows_dev + BLOCK * point_row + half_block).astype(jnp.float32)
    pcol = (tile_ref[0] * COLS + BLOCK * point_col + half_block).astype(jnp.float32)
    for b in range(blocks):
        ref = pieces[b // per_piece]
        lanes = slice((b % per_piece) * LANES, (b % per_piece + 1) * LANES)
        ens = ref[0:members, lanes]
        centre = jnp.sum(ens, axis=0, keepdims=True) / members
        ens_ref[b, 0:members, :] = ens - centre
        meta = ref[members : members + 4, lanes]
        ens_ref[b, members : members + 1, :] = meta[0:1] - centre
        row_gap = jnp.abs(meta[2:3] - prow)
        col_gap = jnp.abs(meta[3:4] - pcol)
        col_gap = jnp.minimum(col_gap, circle - col_gap)
        taper = jnp.maximum(0.0, 1.0 - row_gap / extent) * jnp.maximum(0.0, 1.0 - col_gap / extent)
        weight = taper * meta[1:2]
        weight_ref[b] = weight
        live_ref[b] = (jnp.max(weight) > 0.0).astype(jnp.int32)
    gram_ref[...] = jnp.zeros(gram_ref.shape, jnp.float32)
    fill = jnp.zeros((LANES - members, 2 * LANES), jnp.bfloat16)
    blank = jnp.zeros((members, LANES), jnp.bfloat16)

    def visit(b, carry):
        @pl.when(live_ref[b] > 0)
        def _():
            spread = ens_ref[b, 0:members, :]
            innovation = ens_ref[b, members : members + 1, :]
            weight = weight_ref[b]
            high, low = halves(spread)
            right = jnp.concatenate(
                [
                    jnp.concatenate([high, high], axis=1),
                    fill,
                    jnp.concatenate([low, blank], axis=1),
                    fill,
                ],
                axis=0,
            )
            left = []
            for p in range(points):
                left.append(jnp.concatenate(halves(weight[p : p + 1] * spread), axis=1))
            left.append(jnp.concatenate(halves(weight * innovation), axis=1))
            gram_ref[...] += dot_nt(jnp.concatenate(left, axis=0), right)

        return carry

    lax.fori_loop(0, blocks, visit, 0)

    row_id = lax.broadcasted_iota(jnp.int32, (members, LANES), 0)
    lane_id = lax.broadcasted_iota(jnp.int32, (members, LANES), 1)
    identity = jnp.where(row_id == lane_id, 1.0, 0.0)
    middle_id = 1.5 * identity

    def left_of(parts):
        return jnp.concatenate(parts, axis=1)

    def right_of(parts):
        high, low = parts
        return jnp.concatenate(
            [
                jnp.concatenate([high, low], axis=1),
                fill,
                jnp.concatenate([high, blank], axis=1),
                fill,
            ],
            axis=0,
        )

    def folded(x):
        return x[:, :LANES] + x[:, LANES:]

    norms = []
    for p in range(points):
        gram = folded(gram_ref[p * members : (p + 1) * members, :]) + (members - 1.0) * identity
        squares = jnp.sum(jnp.sum(gram * gram, axis=0, keepdims=True), axis=1, keepdims=True)
        norm = jnp.sqrt(squares)
        norms.append(norm)
        iter_ref[p] = gram / norm
    for p in range(points):
        iterate = iter_ref[p]
        middle = middle_id - 0.5 * iterate
        iter_ref[p] = folded(dot_nn(left_of(halves(iterate)), right_of(halves(middle))))
        root_ref[p] = middle
    for sweep in range(1, NS_ITERS):
        last = sweep == NS_ITERS - 1
        for p in range(points):
            root = halves(root_ref[p])
            iterate = halves(iter_ref[p])
            product = folded(dot_nn(left_of(root), right_of(iterate)))
            middle = right_of(halves(middle_id - 0.5 * product))
            if last:
                root_ref[p] = folded(dot_nn(left_of(root), middle))
            else:
                both = jnp.concatenate([left_of(root), left_of(iterate)], axis=0)
                both = folded(dot_nn(both, middle))
                root_ref[p] = both[0:members]
                iter_ref[p] = both[members:]
    rhs_all = folded(gram_ref[points * members : points * members + pad_points, :])
    scale = (members - 1.0) ** 0.5
    for p in range(points):
        root = root_ref[p] / jnp.sqrt(norms[p])
        inner = jnp.sum(root * rhs_all[p : p + 1], axis=1, keepdims=True)
        shift = jnp.sum(root * inner, axis=0, keepdims=True)
        high, low = halves(scale * root + shift)
        mix_ref[p * members : (p + 1) * members, 0:LANES] = high
        mix_ref[p * members : (p + 1) * members, LANES:] = low


def apply_body(mix_ref, state_ref, out_ref, *, rows_dev):
    members = state_ref.shape[0]
    col_blocks = COLS // BLOCK
    row_blocks = rows_dev // BLOCK
    cells = state_ref.shape[2]
    state = state_ref[:, 0, :]
    centre = jnp.sum(state, axis=0, keepdims=True) / members
    spread = state - centre
    wide = -(-cells // LANES) * LANES
    band_half = BLOCK * COLS
    results = []
    for r in range(row_blocks):
        start = r * band_half // LANES * LANES
        stop = min(wide, -(-(r + 1) * band_half // LANES) * LANES)
        part = spread[:, start : min(stop, cells)]
        width = part.shape[1]
        high, low = halves(part)
        hole = jnp.zeros((LANES - members, width), jnp.bfloat16)
        top = jnp.concatenate([high, hole, high, hole], axis=0)
        bottom = jnp.concatenate([low, hole], axis=0)
        mix = mix_ref[r * col_blocks * members : (r + 1) * col_blocks * members, :]
        product = dot_nn(mix, top) + dot_nn(mix[:, :LANES], bottom)
        cell = lax.broadcasted_iota(jnp.int32, (members, width), 1) + start
        column = lax.rem(cell, COLS) // BLOCK
        result = centre[:, start : start + width]
        for cb in range(col_blocks):
            result = result + jnp.where(column == cb, product[cb * members : (cb + 1) * members], 0.0)
        results.append((start, width, cell, result))
    if row_blocks == 2:
        (s0, w0, c0, r0), (s1, w1, c1, r1) = results
        out_ref[:, 0, 0:s1] = r0[:, 0:s1]
        joint = jnp.where(c0[:, s1:] < band_half, r0[:, s1:], r1[:, 0 : s0 + w0 - s1])
        out_ref[:, 0, s1 : s0 + w0] = joint
        out_ref[:, 0, s0 + w0 : cells] = r1[:, s0 + w0 - s1 :]


def mixing(extent, band_id, tile_id, own, near, members, circle, rows_dev):
    slots = own.shape[1]
    blocks = (1 + near.shape[0] * (near.shape[1] // PIECE_ROWS)) * slots // LANES
    points = rows_dev // BLOCK * (COLS // BLOCK)
    smem = pl.BlockSpec(memory_space=pltpu.SMEM)
    vmem = pl.BlockSpec(memory_space=pltpu.VMEM)

    def body(*refs):
        mixing_body(*refs, members=members, circle=circle, rows_dev=rows_dev)

    return pl.pallas_call(
        body,
        out_shape=pltpu.VMEM((points * members, 2 * LANES), jnp.bfloat16),
        in_specs=[smem] * 3 + [vmem] * 2,
        out_specs=vmem,
        scratch_shapes=[
            pltpu.VMEM((blocks, PIECE_ROWS, LANES), jnp.float32),
            pltpu.VMEM((blocks, 16, LANES), jnp.float32),
            pltpu.SMEM((blocks,), jnp.int32),
            pltpu.VMEM((points * members + 16, 2 * LANES), jnp.float32),
            pltpu.VMEM((points, members, LANES), jnp.float32),
            pltpu.VMEM((points, members, LANES), jnp.float32),
        ],
        name="mixing",
    )(extent, band_id, tile_id, on_chip(own), on_chip(near))


def applied(mix, state, rows_dev):
    vmem = pl.BlockSpec(memory_space=pltpu.VMEM)

    def body(*refs):
        apply_body(*refs, rows_dev=rows_dev)

    return pl.pallas_call(
        body,
        out_shape=pltpu.VMEM(state.shape, jnp.float32),
        in_specs=[vmem] * 2,
        out_specs=vmem,
        name="applied",
    )(on_chip(mix), on_chip(state))


def fetched(block, distance):
    tiles = lax.axis_size("tile")
    route = []
    for group in range(lax.axis_size("mem")):
        step = distance if group % 2 == 0 else -distance
        route += [(group * tiles + (t - step) % tiles, group * tiles + t) for t in range(tiles)]
    return lax.ppermute(block, ("mem", "tile"), route)


def shards(state, obs_index, obs_count, obs_value, obs_rinv, radius):
    groups = lax.axis_size("mem")
    tile_count = lax.axis_size("tile")
    mem_dev = state.shape[0]
    cell_count = state.shape[2]
    members = mem_dev * groups
    band_cells = cell_count // groups
    rows_dev = band_cells // COLS
    circle = 1.0 * COLS * tile_count
    tile_id = lax.axis_index("tile")
    band_id = lax.axis_index("mem")
    slot_count = obs_index.shape[1]
    tile_at = tile_id.reshape(1)
    copies, meta = take_cells(obs_count, tile_at, state, obs_index, obs_value, obs_rinv, groups)
    ensemble = lax.all_to_all(copies, "mem", 0, 0, tiled=True)
    ensemble = ensemble.reshape(members, slot_count)
    chunks = state.reshape(mem_dev, groups, band_cells).transpose(1, 0, 2)
    chunks = chunks.reshape(members, 1, band_cells)
    band_state = lax.all_to_all(chunks, "mem", 0, 0, tiled=True)
    extent = (radius * COLS).astype(jnp.float32)
    own = jnp.concatenate([ensemble, meta], axis=0)
    half = []
    for distance in range(1, HALO + 1):
        half.append(fetched(own, distance))
    half = jnp.concatenate(half, axis=0)
    pairs = [[group, group + 1] for group in range(0, groups, 2)]
    near = lax.all_gather(half, "mem", axis_index_groups=pairs)
    mix = mixing(extent, band_id.reshape(1), tile_at, own, near, members, circle, rows_dev)
    result = applied(mix, band_state, rows_dev)
    returned = lax.all_to_all(result, "mem", 0, 0, tiled=True)
    returned = returned.reshape(groups, mem_dev, band_cells).transpose(1, 0, 2)
    return returned.reshape(mem_dev, 1, cell_count)


def solution(mesh):
    in_specs = (
        P("mem", "tile", None),
        P("tile", None),
        P("tile"),
        P("tile", None),
        P("tile", None),
        P("tile"),
    )
    out_specs = P("mem", "tile", None)
    return jax.shard_map(shards, mesh=mesh, in_specs=in_specs, out_specs=out_specs, check_vma=False)
```
